16 devices in a mesh: rep: 2 (over y, z), dp: 8 (over x, core).
Axes of the slice: x: 4, y: 2, z: 1, core: 2. Of those that a mesh axis runs over, the one named last changes fastest.
The devices are a block of a 4x4x8 slice.
Arguments:
- x: bfloat16 [16, 1024, 1024], P(('rep', 'dp')), parts along dimension 0
- dy: bfloat16 [16, 1024, 1024], P(('rep', 'dp')), parts along dimension 0
- w_gate: bfloat16 [2, 1024, 3200], replicated
- w_up: bfloat16 [2, 1024, 3200], replicated
- w_down: bfloat16 [2, 3200, 1024], replicated
- m_w_gate: float32 [2, 1024, 3200], replicated
- m_w_up: float32 [2, 1024, 3200], replicated
- m_w_down: float32 [2, 3200, 1024], replicated
- v_w_gate: float32 [2, 1024, 3200], replicated
- v_w_up: float32 [2, 1024, 3200], replicated
- v_w_down: float32 [2, 3200, 1024], replicated
Outputs:
- output 1: bfloat16 [4, 1024, 3200], P('rep'), parts along dimension 0
- output 2: bfloat16 [4, 1024, 3200], P('rep'), parts along dimension 0
- output 3: bfloat16 [4, 3200, 1024], P('rep'), parts along dimension 0
- output 4: float32 [4, 1024, 3200], P('rep'), parts along dimension 0
- output 5: float32 [4, 1024, 3200], P('rep'), parts along dimension 0
- output 6: float32 [4, 3200, 1024], P('rep'), parts along dimension 0
- output 7: float32 [4, 1024, 3200], P('rep'), parts along dimension 0
- output 8: float32 [4, 1024, 3200], P('rep'), parts along dimension 0
- output 9: float32 [4, 3200, 1024], P('rep'), parts along dimension 0
There are 2 independent parts. The reference program is written for one: setup_inputs(seed, part) draws one part's arguments, and reference() takes and returns one part's arrays. A program takes and returns all parts, laid end to end along the dimension named above; an argument that names none is the same for every part.
All inputs are finite; a program needn't handle non-finite values.
Results may differ from the reference program's by a relative error of at most 0.022.
Values are sent between devices in bfloat16 or wider.
A program may use at most 768 MiB of HBM per device.

```python
import jax
import jax.numpy as jnp
from jax import lax

SEQUENCES = 8
TOKENS = 1024
D = 1024
FF = 3200
LAYERS = 2
NAMES = ("w_gate", "w_up", "w_down")
SHAPES = {"w_gate": (LAYERS, D, FF), "w_up": (LAYERS, D, FF), "w_down": (LAYERS, FF, D)}


def bump(key, n, height):
    away = (jnp.arange(n, dtype=jnp.int32) - jax.random.randint(key, (), 0, n, jnp.int32)) % n
    return jnp.where(away < n // 8, height, 1.0)


def together(key, own, strength):
    shared = jax.random.normal(key, own.shape[1:], jnp.float32)
    return (own + strength * shared) * lax.rsqrt(1 + strength * strength)


def setup_inputs(seed: int = 0, part: int = 0) -> dict:
    kx, kdy, ka, kb, kz, kf, kh, kl, *keys = jax.random.split(jax.random.key(seed), 8 + 3 * len(NAMES))
    kx, kdy, ka, kb = (jax.random.fold_in(k, part) for k in (kx, kdy, ka, kb))
    kw, km, kv = (keys[i::3] for i in range(3))
    shape = (SEQUENCES, TOKENS, D)
    much_x, much_dy = jax.random.uniform(kz, (2,), jnp.float32, 0.0, 1.0)
    loud = 2.0 ** jax.random.uniform(jax.random.fold_in(kz, 1), (), jnp.float32, -1.0, 2.0)
    layers = 2.0 ** jax.random.uniform(kl, (LAYERS, 1, 1), jnp.float32, -1.0, 1.0)
    x = together(ka, jax.random.normal(kx, shape, jnp.float32), much_x) * bump(kf, D, 4.0)
    dy = together(kb, jax.random.normal(kdy, shape, jnp.float32), much_dy)
    drawn = {"x": x.astype(jnp.bfloat16), "dy": (loud * dy * (SEQUENCES * TOKENS) ** -0.5).astype(jnp.bfloat16)}
    for key, name in zip(kw, NAMES, strict=True):
        w = jax.random.normal(key, SHAPES[name], jnp.float32) * SHAPES[name][1] ** -0.5
        drawn[name] = (w * {"w_gate": 1.0, "w_up": bump(kh, FF, 4.0), "w_down": layers}[name]).astype(jnp.bfloat16)
    for key, name in zip(km, NAMES, strict=True):
        drawn[f"m_{name}"] = 0.1 * jax.random.normal(key, SHAPES[name], jnp.float32)
    for key, name in zip(kv, NAMES, strict=True):
        drawn[f"v_{name}"] = jax.random.uniform(key, SHAPES[name], jnp.float32, 0.005, 0.015)
    return drawn


def matmul(a, w):
    return jnp.dot(a, w, preferred_element_type=jnp.float32).astype(jnp.bfloat16)


def normed(h):
    wide = h.astype(jnp.float32)
    scale = lax.rsqrt(jnp.mean(wide**2, -1, keepdims=True) + 1e-6)
    return (wide * scale).astype(jnp.bfloat16)


def layer(h, w):
    a = normed(h)
    gate = jnp.dot(a, w["w_gate"], preferred_element_type=jnp.float32)
    up = jnp.dot(a, w["w_up"], preferred_element_type=jnp.float32)
    return h + matmul((jax.nn.silu(gate) * up).astype(jnp.bfloat16), w["w_down"])


def adamw(w, m, v, g):
    m = 0.9 * m + 0.1 * g
    v = 0.95 * v + 0.05 * g * g
    step = m * lax.rsqrt(v + 1e-8) + 0.1 * w
    return (w - 0.02 * step).astype(jnp.bfloat16), m, v


def clipped(gradients, sum_of_squares, count):
    factor = jnp.minimum(1.0, 0.5 * lax.rsqrt(sum_of_squares / count + 1e-30))
    return [g * factor for g in gradients]


def stack(weights, h):
    return lax.scan(lambda h, w: (layer(h, w), None), h, weights)[0]


def reference(x, dy, w_gate, w_up, w_down, m_w_gate, m_w_up, m_w_down, v_w_gate, v_w_up, v_w_down):
    weights = dict(zip(NAMES, (w_gate, w_up, w_down), strict=True))

    def take(so_far, sequence):
        h, by_y = sequence
        _, back = jax.vjp(lambda w: stack(w, h), weights)
        return jax.tree.map(lambda total, term: total + term.astype(jnp.float32), so_far, back(by_y)[0]), None

    none_yet = {name: jnp.zeros(w.shape, jnp.float32) for name, w in weights.items()}
    by_weights, _ = lax.scan(take, none_yet, (x, dy))
    gradients = [by_weights[name].astype(jnp.bfloat16).astype(jnp.float32) for name in NAMES]
    gradients = clipped(gradients, sum(jnp.sum(g * g) for g in gradients), sum(g.size for g in gradients))
    new = [
        adamw(w.astype(jnp.float32), m, v, g)
        for w, m, v, g in zip((w_gate, w_up, w_down), (m_w_gate, m_w_up, m_w_down), (v_w_gate, v_w_up, v_w_down), gradients, strict=True)
    ]
    return tuple(one[which] for which in range(3) for one in new)
```

```python
import functools

import jax
import jax.numpy as jnp
from jax import lax
from jax.experimental import pallas as pl
from jax.experimental.pallas import tpu as pltpu
from jax.sharding import PartitionSpec as P

NAMES = ("w_gate", "w_up", "w_down")
SLOTS = 4


def matmul(a, w):
    return jnp.dot(a, w, preferred_element_type=jnp.float32).astype(jnp.bfloat16)


def normed(h):
    wide = h.astype(jnp.float32)
    scale = lax.rsqrt(jnp.mean(wide**2, -1, keepdims=True) + 1e-6)
    return (wide * scale).astype(jnp.bfloat16)


def layer(h, w):
    a = normed(h)
    gate = jnp.dot(a, w["w_gate"], preferred_element_type=jnp.float32)
    up = jnp.dot(a, w["w_up"], preferred_element_type=jnp.float32)
    return h + matmul((jax.nn.silu(gate) * up).astype(jnp.bfloat16), w["w_down"])


MESH = pl.DeviceIdType.MESH
DEEP = 3
TILES = 5


def hops():
    me = lax.axis_index("dp")
    c, x = me % 2, me // 2
    a = x + 1 - 2 * (x % 2)
    return me, c, x, a, 3 - x, 3 - a


def backward_kernel(
    n, layers, x_ref, *refs
):
    inner, refs = refs[: layers - 1], refs[layers - 1 :]
    dy_ref, wg_ref, wu_ref, wd_ref, refs = *refs[:4], refs[4:]
    gu_outs, d_outs, factor_ref, refs = refs[:layers], refs[layers : 2 * layers], refs[2 * layers], refs[2 * layers + 1 :]
    (h, a, aT, dh, dhT, wg, wu, wd, act, dgate, dup, acc_g, acc_u, send0, own, rcv0, rcv1, rcv2, fin, squares, parts,
     w_sem, h_sem, send0_sem, rcv0_sem, send1_sem, rcv1_sem, send2_sem, rcv2_sem, fin_sem, ssend_sem, srecv_sem,
     credit_p, credit_a, credit_b) = refs
    me, c, x, xa, xb, xo = hops()
    peer, to_a, to_b = 2 * x + 1 - c, 2 * xa + c, 2 * xb + c
    tokens, depth = h.shape
    width = wg.shape[-1]
    steps = layers * TILES
    half = depth // 2
    tall = 256
    inputs = (x_ref, *inner)

    def load_h(number):
        return pltpu.make_async_copy(inputs[number], h, h_sem.at[0])

    def weights_of(s):
        number, j, slot = layers - 1 - s // TILES, s % TILES, s % 2
        at = pl.ds(pl.multiple_of(j * width, width), width)
        return [
            pltpu.make_async_copy(wg_ref.at[number, :, at], wg.at[slot], w_sem.at[0, slot]),
            pltpu.make_async_copy(wu_ref.at[number, :, at], wu.at[slot], w_sem.at[1, slot]),
            pltpu.make_async_copy(wd_ref.at[number, at], wd.at[slot], w_sem.at[2, slot]),
        ]

    def turn(source, target):
        @pl.loop(0, tokens // 128)
        def _(r):
            at = pl.ds(pl.multiple_of(r * 128, 128), 128)
            target[:, at] = source[at, :].T

    def norm():
        @pl.loop(0, tokens // 64)
        def _(r):
            at = pl.ds(pl.multiple_of(r * 64, 64), 64)
            wide = h[at].astype(jnp.float32)
            scale = lax.rsqrt(jnp.mean(wide**2, -1, keepdims=True) + 1e-6)
            a[at] = (wide * scale).astype(jnp.bfloat16)

    load_h(layers - 1).start()
    first_dh = pltpu.make_async_copy(dy_ref, dh, h_sem.at[1])
    first_dh.start()
    for one in weights_of(0):
        one.start()

    barrier = pltpu.get_barrier_semaphore()
    for k in range(1, n):
        pl.semaphore_signal(barrier, inc=1, device_id={"dp": (me + k) % n}, device_id_type=MESH)
    pl.semaphore_wait(barrier, n - 1)

    load_h(layers - 1).wait()
    norm()
    turn(a, aT)
    first_dh.wait()
    turn(dh, dhT)

    def remote(source, target, sends, receives, to):
        return pltpu.make_async_remote_copy(
            src_ref=source, dst_ref=target, send_sem=sends, recv_sem=receives, device_id={"dp": to}, device_id_type=MESH
        )

    def swap(s):
        return remote(send0.at[s % 2], rcv0.at[s % DEEP], send0_sem.at[s % 2], rcv0_sem.at[s % DEEP], peer)

    def step_one(s):
        k = s % DEEP
        blocks = ((2 * xa, to_a), (2 * xo, to_a), (2 * xb + 1, to_b), (2 * xo + 1, to_b))
        return [(b, remote(own.at[k, b], rcv1.at[k, i], send1_sem.at[k, i], rcv1_sem.at[k, i], to)) for i, (b, to) in enumerate(blocks)]

    def step_two(s):
        k = s % DEEP
        blocks = ((2 * xb, to_b, 1), (2 * xa + 1, to_a, 3))
        return [
            (b, got, remote(own.at[k, b], rcv2.at[k, i], send2_sem.at[k, i], rcv2_sem.at[k, i], to)) for i, (b, to, got) in enumerate(blocks)
        ]

    def summed(s, b, more):
        k = s % DEEP
        for mat in range(3):
            for r in range(0, own.shape[-2], 16):
                at = pl.ds(r, 16)
                total = own[k, b, mat, at].astype(jnp.float32) + rcv0[k, b, mat, at].astype(jnp.float32)
                for ref, i in more:
                    total = total + ref[k, i, mat, at].astype(jnp.float32)
                yield mat, at, total.astype(jnp.bfloat16)

    def begin(s):
        swap(s).wait_recv()

        @pl.when(s >= DEEP)
        def _():
            pl.semaphore_wait(credit_a, 1)
            pl.semaphore_wait(credit_b, 1)

        copies = step_one(s)
        for b, _ in copies:
            for mat, at, total in summed(s, b, ()):
                own[s % DEEP, b, mat, at] = total
        for _, one in copies:
            one.start()

    def pass_on(s):
        for _, one in step_one(s):
            one.wait_recv()
        copies = step_two(s)
        for b, got, _ in copies:
            for mat, at, total in summed(s, b, ((rcv1, got),)):
                own[s % DEEP, b, mat, at] = total
        for *_, one in copies:
            one.start()

    def fin_copies(s, number):
        at = pl.ds(pl.multiple_of((s % TILES) * width, width), width)
        return [
            pltpu.make_async_copy(fin.at[:, 0:2], gu_outs[number].at[:, :, :, at], fin_sem.at[0]),
            pltpu.make_async_copy(fin.at[:, 2], d_outs[number].at[:, :, at], fin_sem.at[1]),
        ]

    def finish(s):
        for *_, one in step_two(s):
            one.wait_recv()

        @pl.when(s >= 1)
        def _():
            for one in fin_copies(s, 0):
                one.wait()

        for colour in range(2):
            for mat, at, total in summed(s, 2 * x + colour, ((rcv1, 2 * colour), (rcv2, colour))):
                fin[colour, mat, at] = total
                squared = total.astype(jnp.float32) ** 2
                squares[...] += squared[:8] + squared[8:]
        for number in range(layers):

            @pl.when(layers - 1 - s // TILES == number)
            def _():
                for one in fin_copies(s, number):
                    one.start()

        for _, one in step_one(s):
            one.wait_send()
        for *_, one in step_two(s):
            one.wait_send()

        @pl.when(s + DEEP < steps)
        def _():
            pl.semaphore_signal(credit_p, inc=1, device_id={"dp": peer}, device_id_type=MESH)
            pl.semaphore_signal(credit_a, inc=1, device_id={"dp": to_a}, device_id_type=MESH)
            pl.semaphore_signal(credit_b, inc=1, device_id={"dp": to_b}, device_id_type=MESH)

    def gradients(core, keep):
        for_rows = half // tall

        @pl.loop(0, for_rows)
        def _(r):
            at = pl.ds(pl.multiple_of(core * half + r * tall, tall), tall)
            blocks = tall // 64
            for mat, (left, right) in enumerate(((aT, dgate), (aT, dup), (dhT, act))):
                got = jnp.dot(left[at], right[...], preferred_element_type=jnp.float32).astype(jnp.bfloat16)
                for b in range(blocks):
                    keep(r * blocks + b, mat, got[b * 64 : (b + 1) * 64])

    squares[...] = jnp.zeros_like(squares)

    @pl.loop(0, steps)
    def _(s):
        slot, k = s % 2, s % DEEP
        for one in weights_of(s):
            one.wait()

        @pl.when(s + 1 < steps)
        def _():
            for one in weights_of(s + 1):
                one.start()

        @pl.loop(0, tokens // tall)
        def _(r):
            at = pl.ds(pl.multiple_of(r * tall, tall), tall)
            gate = jnp.dot(a[at], wg[slot], preferred_element_type=jnp.float32)
            up = jnp.dot(a[at], wu[slot], preferred_element_type=jnp.float32)
            by_act = lax.dot_general(dh[at], wd[slot], (((1,), (1,)), ((), ())), preferred_element_type=jnp.float32)
            by_act = by_act.astype(jnp.bfloat16).astype(jnp.float32)
            share = jax.nn.sigmoid(gate)
            silu = gate * share
            act[at] = (silu * up).astype(jnp.bfloat16)
            dup[at] = (by_act * silu).astype(jnp.bfloat16)
            dgate[at] = (by_act * up * (share + silu * (1.0 - share))).astype(jnp.bfloat16)

        @pl.when(s >= 2)
        def _():
            swap(s).wait_send()

        def to_send(b, mat, value):
            send0[slot, b, mat] = value

        gradients(1 - c, to_send)

        @pl.when(s >= DEEP)
        def _():
            pl.semaphore_wait(credit_p, 1)

        swap(s).start()

        def to_own(b, mat, value):
            own[k, b, mat] = value

        gradients(c, to_own)
        begin(s)

        @pl.when(s >= 1)
        def _():
            pass_on(s - 1)

        @pl.when(s >= 2)
        def _():
            finish(s - 2)

        @pl.when(s < steps - TILES)
        def _():
            @pl.when(s % TILES == 0)
            def _():
                acc_g[...] = jnp.zeros_like(acc_g)
                acc_u[...] = jnp.zeros_like(acc_u)

            @pl.loop(0, tokens // tall)
            def _(r):
                at = pl.ds(pl.multiple_of(r * tall, tall), tall)
                for total, by, w in ((acc_g, dgate, wg), (acc_u, dup, wu)):
                    total[at] += lax.dot_general(by[at], w[slot], (((1,), (1,)), ((), ())), preferred_element_type=jnp.float32)

            @pl.when(s % TILES == TILES - 1)
            def _():
                @pl.loop(0, tokens // 32)
                def _(r):
                    at = pl.ds(pl.multiple_of(r * 32, 32), 32)
                    by = acc_g[at].astype(jnp.bfloat16) + acc_u[at].astype(jnp.bfloat16)
                    by, wide = by.astype(jnp.float32), h[at].astype(jnp.float32)
                    scale = lax.rsqrt(jnp.mean(wide**2, -1, keepdims=True) + 1e-6)
                    inner = jnp.mean(by * wide, -1, keepdims=True)
                    by_h = (by * scale - wide * (scale * scale * scale * inner)).astype(jnp.bfloat16)
                    dh[at] = dh[at] + by_h

                for number in range(layers - 1):

                    @pl.when(layers - 2 - s // TILES == number)
                    def _():
                        load_h(number).start()
                        load_h(number).wait()

                norm()
                turn(a, aT)
                turn(dh, dhT)

    pass_on(jnp.int32(steps - 1))
    finish(jnp.int32(steps - 2))
    finish(jnp.int32(steps - 1))
    for one in fin_copies(jnp.int32(steps - 1), 0):
        one.wait()
    swap(jnp.int32(steps - 2)).wait_send()
    swap(jnp.int32(steps - 1)).wait_send()

    parts[me] = sum(squares[:, k * 128 : (k + 1) * 128] for k in range(width // 128))

    def share(k):
        return remote(parts.at[me], parts.at[me], ssend_sem.at[k], srecv_sem.at[k], (me + k) % n)

    for k in range(1, n):
        share(k).start()
    for k in range(1, n):
        share(k).wait()
    total = parts[0]
    for k in range(1, n):
        total = total + parts[k]
    count = steps * width * depth * 3
    factor_ref[...] = jnp.minimum(1.0, 0.5 * lax.rsqrt(jnp.full(factor_ref.shape, jnp.sum(total)) / count + 1e-30))


def backward(n, inputs, dy, weights):
    layers, depth, hidden = weights[0].shape
    tokens, width, rows = dy.shape[0], hidden // TILES, depth // 16
    bf16, dma, regular = jnp.bfloat16, pltpu.SemaphoreType.DMA, pltpu.SemaphoreType.REGULAR
    any_spec = pl.BlockSpec(memory_space=pl.ANY)
    out = pl.pallas_call(
        functools.partial(backward_kernel, n, layers),
        out_shape=[jax.ShapeDtypeStruct((2, 2, rows, hidden), bf16)] * layers
        + [jax.ShapeDtypeStruct((2, rows, hidden), bf16)] * layers
        + [jax.ShapeDtypeStruct((8, 128), jnp.float32)],
        in_specs=[any_spec] * (layers + 4),
        out_specs=[any_spec] * (2 * layers) + [pl.BlockSpec(memory_space=pltpu.VMEM)],
        scratch_shapes=[
            pltpu.VMEM((tokens, depth), bf16),
            pltpu.VMEM((tokens, depth), bf16),
            pltpu.VMEM((depth, tokens), bf16),
            pltpu.VMEM((tokens, depth), bf16),
            pltpu.VMEM((depth, tokens), bf16),
            pltpu.VMEM((2, depth, width), bf16),
            pltpu.VMEM((2, depth, width), bf16),
            pltpu.VMEM((2, width, depth), bf16),
            pltpu.VMEM((tokens, width), bf16),
            pltpu.VMEM((tokens, width), bf16),
            pltpu.VMEM((tokens, width), bf16),
            pltpu.VMEM((tokens, depth), jnp.float32),
            pltpu.VMEM((tokens, depth), jnp.float32),
            pltpu.VMEM((2, 8, 3, rows, width), bf16),
            pltpu.VMEM((DEEP, 8, 3, rows, width), bf16),
            pltpu.VMEM((DEEP, 8, 3, rows, width), bf16),
            pltpu.VMEM((DEEP, 4, 3, rows, width), bf16),
            pltpu.VMEM((DEEP, 2, 3, rows, width), bf16),
            pltpu.VMEM((2, 3, rows, width), bf16),
            pltpu.VMEM((8, width), jnp.float32),
            pltpu.VMEM((n, 8, 128), jnp.float32),
            dma((3, 2)),
            dma((2,)),
            dma((2,)),
            dma((DEEP,)),
            dma((DEEP, 4)),
            dma((DEEP, 4)),
            dma((DEEP, 2)),
            dma((DEEP, 2)),
            dma((2,)),
            dma((n,)),
            dma((n,)),
            regular,
            regular,
            regular,
        ],
        compiler_params=pltpu.CompilerParams(collective_id=0, has_side_effects=True, vmem_limit_bytes=67_043_328),
        cost_estimate=pl.CostEstimate(flops=16 * tokens * depth * hidden * layers, bytes_accessed=2**27, transcendentals=0),
    )(*inputs, dy, *weights)
    return out[:layers], out[layers : 2 * layers], out[-1]


def update_kernel(items, n_new, *refs):
    n_g = 1 + max(item[0] for item in items)
    factor_ref, refs = refs[0], refs[1:]
    g_refs, refs = refs[:n_g], refs[n_g:]
    old, refs = refs[:9], refs[9:]
    if not n_new:
        refs = refs[9:]
    new, refs = refs[:9], refs[9:]
    factor_vmem, wide, tall, in_sem, out_sem, f_sem = refs
    c, x = place()
    copy = pltpu.make_async_copy(factor_ref, factor_vmem, f_sem)
    copy.start()
    copy.wait()
    factor = factor_vmem[0:1, 0:1]

    def views(n):
        which, tile, weight, layer, core, rel, colour = items[n]
        slot = n % SLOTS
        buffers = [b.at[slot] for b in (tall if weight == 2 else wide)]
        rows, cols = buffers[0].shape
        owner = spot(c, x, core, rel)
        if weight == 2:
            index = (layer, pl.ds(colour * rows, rows), pl.ds(pl.multiple_of(owner * cols, cols), cols))
        else:
            index = (layer, pl.ds(pl.multiple_of((owner * 2 + colour) * rows, rows), rows))
        sources = [old[3 * j + weight].at[index] for j in range(3)] + [g_refs[which].at[tile]]
        targets = [new[3 * j + weight].at[index] for j in range(3)]
        return buffers, sources, targets, slot

    def loads(n):
        buffers, sources, _, slot = views(n)
        return [pltpu.make_async_copy(s, b, in_sem.at[j, slot]) for j, (s, b) in enumerate(zip(sources, buffers, strict=True))]

    def stores(n):
        buffers, _, targets, slot = views(n)
        return [pltpu.make_async_copy(b, t, out_sem.at[j, slot]) for j, (b, t) in enumerate(zip(buffers[:3], targets, strict=True))]

    ahead = SLOTS - 2
    for n in range(min(ahead, len(items))):
        for one in loads(n):
            one.start()
    for n in range(len(items)):
        if n + ahead < len(items):
            if n + ahead - SLOTS >= 0:
                for one in stores(n + ahead - SLOTS):
                    one.wait()
            for one in loads(n + ahead):
                one.start()
        for one in loads(n):
            one.wait()
        w_ref, m_ref, v_ref, g_ref = views(n)[0]
        rows, cols = w_ref.shape
        across = cols // 5 if cols % 5 == 0 else cols

        @pl.loop(0, rows // 16)
        def _(r):
            at = pl.ds(pl.multiple_of(r * 16, 16), 16)
            for k in range(cols // across):
                lanes = pl.ds(k * across, across)
                g = g_ref[at, lanes].astype(jnp.float32) * factor
                m = 0.9 * m_ref[at, lanes] + 0.1 * g
                v = 0.95 * v_ref[at, lanes] + 0.05 * g * g
                w = w_ref[at, lanes].astype(jnp.float32)
                move = m * lax.rsqrt(v + 1e-8) + 0.1 * w
                w_ref[at, lanes] = (w - 0.02 * move).astype(jnp.bfloat16)
                m_ref[at, lanes] = m
                v_ref[at, lanes] = v

        for one in stores(n):
            one.start()
    for n in range(max(0, len(items) - SLOTS), len(items)):
        for one in stores(n):
            one.wait()


def place():
    me = lax.axis_index("dp")
    return me % 2, me // 2


def spot(c, x, core, rel):
    near = x + (rel % 2) * (1 - 2 * (x % 2))
    return (c + core) % 2 * 4 + (3 - near if rel // 2 else near)


def update(factor, items, gs, old, new):
    rows, cols = old[0].shape[1:]
    down_rows, down_cols = old[2].shape[1:]
    wide, tall = (rows // 16, cols), (down_rows // 2, down_cols // 8)

    def slots(shape):
        return [pltpu.VMEM((SLOTS, *shape), t) for t in (jnp.bfloat16, jnp.float32, jnp.float32, jnp.bfloat16)]

    any_spec = pl.BlockSpec(memory_space=pl.ANY)
    n_in = 1 + len(gs) + 9 + (9 if new is not None else 0)
    size = len(items) * wide[0] * wide[1]
    return pl.pallas_call(
        functools.partial(update_kernel, items, new is None),
        out_shape=[jax.ShapeDtypeStruct(o.shape, o.dtype) for o in old],
        in_specs=[any_spec] * n_in,
        out_specs=[any_spec] * 9,
        scratch_shapes=[
            pltpu.VMEM((8, 128), jnp.float32),
            slots(wide),
            slots(tall),
            pltpu.SemaphoreType.DMA((4, SLOTS)),
            pltpu.SemaphoreType.DMA((3, SLOTS)),
            pltpu.SemaphoreType.DMA,
        ],
        input_output_aliases={} if new is None else {n_in - 9 + i: i for i in range(9)},
        cost_estimate=pl.CostEstimate(flops=size * 400, bytes_accessed=size * 22, transcendentals=size),
        compiler_params=pltpu.CompilerParams(vmem_limit_bytes=32 * 2**20),
    )(factor, *gs, *old, *(new if new is not None else ()))


def solution(mesh):
    n = mesh.shape["dp"]
    chips = n // 2
    pair_a = [(2 * x + c, 2 * (x ^ 1) + c) for x in range(chips) for c in range(2)]
    pair_b = [(2 * x + c, 2 * (chips - 1 - x) + c) for x in range(chips) for c in range(2)]
    peers = [(i, i ^ 1) for i in range(n)]
    to_a, to_b, to_peer = (functools.partial(lax.ppermute, axis_name="dp", perm=perm) for perm in (pair_a, pair_b, peers))

    def step(x, dy, *arrays):
        weights = arrays[:3]
        layers = weights[0].shape[0]
        h, kept = x[0], []
        for number in range(layers):
            kept.append(h)
            if number < layers - 1:
                h = layer(h, {name: w[number] for name, w in zip(NAMES, weights, strict=True)})
        wide, tall, factor = backward(n, kept, dy[0], weights)
        shards = []
        for number in reversed(range(layers)):
            down = tall[number].reshape(-1, tall[number].shape[-1]).T
            shards.append((number, 2, down.reshape(2, 1, down.shape[0] // 2, down.shape[1])))
            shards.append((number, 0, wide[number]))

        def run(new, parts):
            items, gs = [], []
            for unit, g, core, rel, colour in parts:
                number, weight, own = shards[unit]
                for this in range(2) if colour is None else (colour,):
                    for kind in range(own.shape[1]):
                        tile = (this, kind) if colour is None else (kind,)
                        items.append((len(gs), tile, weight + kind, number, core, rel, this))
                gs.append(g)
            return update(factor, items, gs, arrays, new)

        def after(new, waited):
            first, waited = lax.optimization_barrier((new[0], waited))
            return [first, *new[1:]], waited

        owns = [own for _, _, own in shards]
        near = [(to_a(own), to_b(own)) for own in owns]
        beside = [to_peer(own) for own in owns]
        new = run(None, [(u, own, 0, 0, None) for u, own in enumerate(owns)] + [(u, g, 1, 0, None) for u, g in enumerate(beside)])
        groups, far = [(0, 1), (2, 3)], []
        for i, group in enumerate(groups):
            new, got = after(new, [near[u] for u in group])
            far.append([(to_a(from_b[0]), to_b(from_a[1])) for from_a, from_b in got])
            beside = [(to_peer(from_a), to_peer(from_b)) for from_a, from_b in got]
            new = run(new, [(u, g, 0, 1 + j, None) for u, pair in zip(group, got, strict=True) for j, g in enumerate(pair)])
            new = run(new, [(u, g, 1, 1 + j, None) for u, pair in zip(group, beside, strict=True) for j, g in enumerate(pair)])
        for i, group in enumerate(groups):
            new, got = after(new, far[i])
            beside = [(to_peer(over_a), to_peer(over_b)) for over_a, over_b in got]
            new = run(new, [(u, g, 0, 3, j) for u, pair in zip(group, got, strict=True) for j, g in enumerate(pair)])
            new = run(new, [(u, g, 1, 3, j) for u, pair in zip(group, beside, strict=True) for j, g in enumerate(pair)])
        return tuple(new)

    return jax.shard_map(
        step,
        mesh=mesh,
        in_specs=(P(("rep", "dp"), None, None),) * 2 + (P(None, None, None),) * 9,
        out_specs=(P("rep", None, None),) * 9,
        check_vma=False,
    )
```

```python
import functools

import jax
import jax.numpy as jnp
from jax import lax
from jax.experimental import pallas as pl
from jax.experimental.pallas import tpu as pltpu
from jax.sharding import PartitionSpec as P


SLOTS = 4


MESH = pl.DeviceIdType.MESH
DEEP = 4
TILES = 5


def hops():
    me = lax.axis_index("dp")
    c, x = me % 2, me // 2
    a = x + 1 - 2 * (x % 2)
    return me, c, x, a, 3 - x, 3 - a


def backward_kernel(
    n, layers, x_ref, dy_ref, wg_ref, wu_ref, wd_ref, *refs
):
    outs, factor_ref, refs = refs[: 2 * layers], refs[2 * layers], refs[2 * layers + 1 :]
    (hs, a, aT, dh, wg, wu, wd, actT, dgate, dup, acc_g, acc_u, send0, own, rcv0, rcv1, rcv2, fin, squares, parts,
     w_sem, h_sem, send0_sem, rcv0_sem, send1_sem, rcv1_sem, send2_sem, rcv2_sem, fin_sem, ssend_sem, srecv_sem,
     credit_p, credit_a, credit_b) = refs
    me, c, x, xa, xb, xo = hops()
    peer, to_a, to_b = 2 * x + 1 - c, 2 * xa + c, 2 * xb + c
    tokens, depth = dh.shape
    width = wg.shape[-1]
    steps = layers * TILES
    half = depth // 2
    ahead = (layers - 1) * TILES
    tall = 512

    def weights_of(t, number):
        j, slot = t % TILES, t % 2
        at = pl.ds(pl.multiple_of(j * width, width), width)
        return [
            pltpu.make_async_copy(wg_ref.at[number, :, at], wg.at[slot], w_sem.at[0, slot]),
            pltpu.make_async_copy(wu_ref.at[number, :, at], wu.at[slot], w_sem.at[1, slot]),
            pltpu.make_async_copy(wd_ref.at[number, at], wd.at[slot], w_sem.at[2, slot]),
        ]

    def turn(source, target):
        @pl.loop(0, tokens // 128)
        def _(r):
            at = pl.ds(pl.multiple_of(r * 128, 128), 128)
            target[:, at] = source[at, :].T

    def norm(h):
        @pl.loop(0, tokens // 64)
        def _(r):
            at = pl.ds(pl.multiple_of(r * 64, 64), 64)
            wide = h[at].astype(jnp.float32)
            scale = lax.rsqrt(jnp.mean(wide**2, -1, keepdims=True) + 1e-6)
            a[at] = (wide * scale).astype(jnp.bfloat16)

    first_h = pltpu.make_async_copy(x_ref, hs.at[0], h_sem.at[0])
    first_h.start()
    first_dh = pltpu.make_async_copy(dy_ref, dh, h_sem.at[1])
    first_dh.start()
    for one in weights_of(0, 0):
        one.start()

    barrier = pltpu.get_barrier_semaphore()
    for k in range(1, n):
        pl.semaphore_signal(barrier, inc=1, device_id={"dp": (me + k) % n}, device_id_type=MESH)
    pl.semaphore_wait(barrier, n - 1)

    first_h.wait()

    for number in range(layers - 1):
        norm(hs.at[number])
        acc_g[...] = jnp.zeros_like(acc_g)

        @pl.loop(number * TILES, (number + 1) * TILES)
        def _(t):
            slot = t % 2
            for one in weights_of(t, number):
                one.wait()
            for one in weights_of(t + 1, (t + 1) // TILES):
                one.start()

            @pl.loop(0, tokens // tall)
            def _(r):
                at = pl.ds(pl.multiple_of(r * tall, tall), tall)
                gate = jnp.dot(a[at], wg[slot], preferred_element_type=jnp.float32)
                up = jnp.dot(a[at], wu[slot], preferred_element_type=jnp.float32)
                dup[at] = (gate * jax.nn.sigmoid(gate) * up).astype(jnp.bfloat16)
                acc_g[at] += jnp.dot(dup[at], wd[slot], preferred_element_type=jnp.float32)

        @pl.loop(0, tokens // 64)
        def _(r):
            at = pl.ds(pl.multiple_of(r * 64, 64), 64)
            hs[number + 1, at] = hs[number, at] + acc_g[at].astype(jnp.bfloat16)

    norm(hs.at[layers - 1])
    turn(a, aT)
    first_dh.wait()

    def remote(source, target, sends, receives, to):
        return pltpu.make_async_remote_copy(
            src_ref=source, dst_ref=target, send_sem=sends, recv_sem=receives, device_id={"dp": to}, device_id_type=MESH
        )

    def swap(s):
        return remote(send0.at[s % 2], rcv0.at[s % DEEP], send0_sem.at[s % 2], rcv0_sem.at[s % DEEP], peer)

    def step_one(s):
        k = s % DEEP
        blocks = ((2 * xa, to_a), (2 * xo, to_a), (2 * xb + 1, to_b), (2 * xo + 1, to_b))
        return [(b, remote(own.at[k, b], rcv1.at[k, i], send1_sem.at[k, i], rcv1_sem.at[k, i], to)) for i, (b, to) in enumerate(blocks)]

    def step_two(s):
        k = s % DEEP
        blocks = ((2 * xb, to_b, 1), (2 * xa + 1, to_a, 3))
        return [
            (b, got, remote(own.at[k, b], rcv2.at[k, i], send2_sem.at[k, i], rcv2_sem.at[k, i], to)) for i, (b, to, got) in enumerate(blocks)
        ]

    def summed(s, b, more):
        k = s % DEEP
        for mat in range(3):
            for r in range(0, own.shape[-2], 16):
                at = pl.ds(r, 16)
                total = own[k, b, mat, at].astype(jnp.float32) + rcv0[k, b, mat, at].astype(jnp.float32)
                for ref, i in more:
                    total = total + ref[k, i, mat, at].astype(jnp.float32)
                yield mat, at, total.astype(jnp.bfloat16)

    def begin(s):
        swap(s).wait_recv()

        @pl.when(s >= DEEP)
        def _():
            pl.semaphore_wait(credit_a, 1)
            pl.semaphore_wait(credit_b, 1)

        copies = step_one(s)
        for b, _ in copies:
            for mat, at, total in summed(s, b, ()):
                own[s % DEEP, b, mat, at] = total
        for _, one in copies:
            one.start()

    def pass_on(s):
        for _, one in step_one(s):
            one.wait_recv()
        copies = step_two(s)
        for b, got, _ in copies:
            for mat, at, total in summed(s, b, ((rcv1, got),)):
                own[s % DEEP, b, mat, at] = total
        for *_, one in copies:
            one.start()

    def fin_copies(s, number):
        at = pl.ds(pl.multiple_of((s % TILES) * width, width), width)
        return [pltpu.make_async_copy(fin.at[colour], outs[2 * number + colour].at[:, :, at], fin_sem.at[colour]) for colour in range(2)]

    def finish(s):
        for *_, one in step_two(s):
            one.wait_recv()

        @pl.when(s >= 1)
        def _():
            for one in fin_copies(s, 0):
                one.wait()

        for colour in range(2):
            for mat, at, total in summed(s, 2 * x + colour, ((rcv1, 2 * colour), (rcv2, colour))):
                fin[colour, mat, at] = total
                squared = total.astype(jnp.float32) ** 2
                squares[...] += squared[:8] + squared[8:]
        for number in range(layers):

            @pl.when(layers - 1 - s // TILES == number)
            def _():
                for one in fin_copies(s, number):
                    one.start()

        for _, one in step_one(s):
            one.wait_send()
        for *_, one in step_two(s):
            one.wait_send()

        @pl.when(s + DEEP < steps)
        def _():
            pl.semaphore_signal(credit_p, inc=1, device_id={"dp": peer}, device_id_type=MESH)
            pl.semaphore_signal(credit_a, inc=1, device_id={"dp": to_a}, device_id_type=MESH)
            pl.semaphore_signal(credit_b, inc=1, device_id={"dp": to_b}, device_id_type=MESH)

    def gradients(core, keep):
        for_rows = half // tall

        @pl.loop(0, for_rows)
        def _(r):
            at = pl.ds(pl.multiple_of(core * half + r * tall, tall), tall)
            blocks = tall // 64
            for mat, right in enumerate((dgate, dup)):
                got = jnp.dot(aT[at], right[...], preferred_element_type=jnp.float32).astype(jnp.bfloat16)
                for b in range(blocks):
                    keep((r * blocks + b, mat), got[b * 64 : (b + 1) * 64])
            rows = width // 2 // for_rows
            at = pl.ds(pl.multiple_of(core * (width // 2) + r * rows, rows), rows)
            got = jnp.dot(actT[at], dh[...], preferred_element_type=jnp.float32).astype(jnp.bfloat16)
            rows = width // 8
            for b in range(blocks):
                for i in range(rows // 16):
                    for k in range(4):
                        row, col = b // 2 * rows + i * 16, b % 2 * (depth // 2) + k * 128
                        place = (r * blocks + b, 2, pl.ds(k * 16, 16), pl.ds(i * 128, 128))
                        keep(place, got[row : row + 16, col : col + 128])

    squares[...] = jnp.zeros_like(squares)

    @pl.loop(0, steps)
    def _(s):
        t, even, k = s + ahead, s % 2, s % DEEP
        slot = t % 2
        for one in weights_of(t, layers - 1 - s // TILES):
            one.wait()

        @pl.when(s + 1 < steps)
        def _():
            for one in weights_of(t + 1, layers - 1 - (s + 1) // TILES):
                one.start()

        @pl.loop(0, tokens // tall)
        def _(r):
            at = pl.ds(pl.multiple_of(r * tall, tall), tall)
            gate = jnp.dot(a[at], wg[slot], preferred_element_type=jnp.float32)
            up = jnp.dot(a[at], wu[slot], preferred_element_type=jnp.float32)
            by_act = lax.dot_general(dh[at], wd[slot], (((1,), (1,)), ((), ())), preferred_element_type=jnp.float32)
            by_act = by_act.astype(jnp.bfloat16).astype(jnp.float32)
            share = jax.nn.sigmoid(gate)
            silu = gate * share
            actT[:, at] = (silu * up).astype(jnp.bfloat16).T
            dup[at] = (by_act * silu).astype(jnp.bfloat16)
            dgate[at] = (by_act * up * (share + silu * (1.0 - share))).astype(jnp.bfloat16)

        @pl.when(s >= 2)
        def _():
            swap(s).wait_send()

        def to_send(place, value):
            send0[even, *place] = value

        gradients(1 - c, to_send)

        @pl.when(s >= DEEP)
        def _():
            pl.semaphore_wait(credit_p, 1)

        swap(s).start()

        def to_own(place, value):
            own[k, *place] = value

        gradients(c, to_own)
        begin(s)

        @pl.when(s >= 1)
        def _():
            pass_on(s - 1)

        @pl.when(s >= DEEP - 1)
        def _():
            finish(s - (DEEP - 1))

        @pl.when(s < steps - TILES)
        def _():
            @pl.when(s % TILES == 0)
            def _():
                acc_g[...] = jnp.zeros_like(acc_g)
                acc_u[...] = jnp.zeros_like(acc_u)

            @pl.loop(0, tokens // tall)
            def _(r):
                at = pl.ds(pl.multiple_of(r * tall, tall), tall)
                for total, by, w in ((acc_g, dgate, wg), (acc_u, dup, wu)):
                    total[at] += lax.dot_general(by[at], w[slot], (((1,), (1,)), ((), ())), preferred_element_type=jnp.float32)

            @pl.when(s % TILES == TILES - 1)
            def _():
                @pl.loop(0, tokens // 32)
                def _(r):
                    at = pl.ds(pl.multiple_of(r * 32, 32), 32)
                    by = acc_g[at].astype(jnp.bfloat16) + acc_u[at].astype(jnp.bfloat16)
                    by, wide = by.astype(jnp.float32), hs[layers - 1 - s // TILES, at].astype(jnp.float32)
                    scale = lax.rsqrt(jnp.mean(wide**2, -1, keepdims=True) + 1e-6)
                    inner = jnp.mean(by * wide, -1, keepdims=True)
                    by_h = (by * scale - wide * (scale * scale * scale * inner)).astype(jnp.bfloat16)
                    dh[at] = dh[at] + by_h

                norm(hs.at[layers - 2 - s // TILES])
                turn(a, aT)

    pass_on(jnp.int32(steps - 1))
    for back in range(DEEP - 1, 0, -1):
        finish(jnp.int32(steps - back))
    for one in fin_copies(jnp.int32(steps - 1), 0):
        one.wait()
    swap(jnp.int32(steps - 2)).wait_send()
    swap(jnp.int32(steps - 1)).wait_send()

    parts[me] = sum(squares[:, k * 128 : (k + 1) * 128] for k in range(width // 128))

    def share(k):
        return remote(parts.at[me], parts.at[me], ssend_sem.at[k], srecv_sem.at[k], (me + k) % n)

    for k in range(1, n):
        share(k).start()
    for k in range(1, n):
        share(k).wait()
    total = parts[0]
    for k in range(1, n):
        total = total + parts[k]
    count = steps * width * depth * 3
    factor_ref[...] = jnp.minimum(1.0, 0.5 * lax.rsqrt(jnp.full(factor_ref.shape, jnp.sum(total)) / count + 1e-30))


def backward(n, x, dy, weights):
    layers, depth, hidden = weights[0].shape
    tokens, width, rows = dy.shape[0], hidden // TILES, depth // 16
    bf16, dma, regular = jnp.bfloat16, pltpu.SemaphoreType.DMA, pltpu.SemaphoreType.REGULAR
    any_spec = pl.BlockSpec(memory_space=pl.ANY)
    out = pl.pallas_call(
        functools.partial(backward_kernel, n, layers),
        out_shape=[jax.ShapeDtypeStruct((3, rows, hidden), bf16)] * (2 * layers)
        + [jax.ShapeDtypeStruct((8, 128), jnp.float32)],
        in_specs=[any_spec] * 5,
        out_specs=[any_spec] * (2 * layers) + [pl.BlockSpec(memory_space=pltpu.VMEM)],
        scratch_shapes=[
            pltpu.VMEM((layers, tokens, depth), bf16),
            pltpu.VMEM((tokens, depth), bf16),
            pltpu.VMEM((depth, tokens), bf16),
            pltpu.VMEM((tokens, depth), bf16),
            pltpu.VMEM((2, depth, width), bf16),
            pltpu.VMEM((2, depth, width), bf16),
            pltpu.VMEM((2, width, depth), bf16),
            pltpu.VMEM((width, tokens), bf16),
            pltpu.VMEM((tokens, width), bf16),
            pltpu.VMEM((tokens, width), bf16),
            pltpu.VMEM((tokens, depth), jnp.float32),
            pltpu.VMEM((tokens, depth), jnp.float32),
            pltpu.VMEM((2, 8, 3, rows, width), bf16),
            pltpu.VMEM((DEEP, 8, 3, rows, width), bf16),
            pltpu.VMEM((DEEP, 8, 3, rows, width), bf16),
            pltpu.VMEM((DEEP, 4, 3, rows, width), bf16),
            pltpu.VMEM((DEEP, 2, 3, rows, width), bf16),
            pltpu.VMEM((2, 3, rows, width), bf16),
            pltpu.VMEM((8, width), jnp.float32),
            pltpu.VMEM((n, 8, 128), jnp.float32),
            dma((3, 2)),
            dma((2,)),
            dma((2,)),
            dma((DEEP,)),
            dma((DEEP, 4)),
            dma((DEEP, 4)),
            dma((DEEP, 2)),
            dma((DEEP, 2)),
            dma((2,)),
            dma((n,)),
            dma((n,)),
            regular,
            regular,
            regular,
        ],
        compiler_params=pltpu.CompilerParams(collective_id=0, has_side_effects=True, vmem_limit_bytes=67_043_328),
        cost_estimate=pl.CostEstimate(flops=16 * tokens * depth * hidden * layers, bytes_accessed=2**27, transcendentals=0),
    )(x, dy, *weights)
    return out[:-1], out[-1]


def update_kernel(items, n_new, *refs):
    n_g = 1 + max(item[0] for item in items)
    factor_ref, refs = refs[0], refs[1:]
    g_refs, refs = refs[:n_g], refs[n_g:]
    old, refs = refs[:9], refs[9:]
    if not n_new:
        refs = refs[9:]
    new, refs = refs[:9], refs[9:]
    factor_vmem, wide, tall, in_sem, out_sem, f_sem = refs
    c, x = place()
    copy = pltpu.make_async_copy(factor_ref, factor_vmem, f_sem)
    copy.start()

    def views(n):
        which, tile, weight, layer, core, rel, colour = items[n]
        slot = n % SLOTS
        buffers = [b.at[slot] for b in (tall if weight == 2 else wide)]
        owner = spot(c, x, core, rel)
        if weight == 2:
            rows, cols = buffers[0].shape[1:]
            index = (layer, slice(None), pl.ds(pl.multiple_of(owner * rows, rows), rows), pl.ds(colour * cols, cols))
        else:
            rows = buffers[0].shape[0]
            index = (layer, pl.ds(pl.multiple_of((owner * 2 + colour) * rows, rows), rows))
        sources = [old[3 * j + weight].at[index] for j in range(3)] + [g_refs[which].at[tile]]
        targets = [new[3 * j + weight].at[index] for j in range(3)]
        return buffers, sources, targets, slot

    def loads(n):
        buffers, sources, _, slot = views(n)
        return [pltpu.make_async_copy(s, b, in_sem.at[j, slot]) for j, (s, b) in enumerate(zip(sources, buffers, strict=True))]

    def stores(n):
        buffers, _, targets, slot = views(n)
        return [pltpu.make_async_copy(b, t, out_sem.at[j, slot]) for j, (b, t) in enumerate(zip(buffers[:3], targets, strict=True))]

    ahead = SLOTS - 2
    for n in range(min(ahead, len(items))):
        for one in loads(n):
            one.start()
    copy.wait()
    factor = factor_vmem[0:1, 0:1]
    for n in range(len(items)):
        if n + ahead < len(items):
            if n + ahead - SLOTS >= 0:
                for one in stores(n + ahead - SLOTS):
                    one.wait()
            for one in loads(n + ahead):
                one.start()
        for one in loads(n):
            one.wait()
        w_ref, m_ref, v_ref, g_ref = views(n)[0]

        def move(place, g):
            g = g.astype(jnp.float32) * factor
            m = 0.9 * m_ref[place] + 0.1 * g
            v = 0.95 * v_ref[place] + 0.05 * g * g
            w = w_ref[place].astype(jnp.float32)
            step = m * lax.rsqrt(v + 1e-8) + 0.1 * w
            w_ref[place] = (w - 0.02 * step).astype(jnp.bfloat16)
            m_ref[place] = m
            v_ref[place] = v

        if items[n][2] == 2:
            tiles, rows = w_ref.shape[:2]

            @pl.loop(0, tiles * (rows // 16))
            def _(r):
                for k in range(g_ref.shape[0] // 16):
                    place = (r // (rows // 16), pl.ds(pl.multiple_of(r % (rows // 16) * 16, 16), 16), pl.ds(k * 128, 128))
                    move(place, g_ref[pl.ds(k * 16, 16), pl.ds(pl.multiple_of(r * 128, 128), 128)])
        else:
            rows, cols = w_ref.shape
            across = cols // TILES

            @pl.loop(0, rows // 16)
            def _(r):
                at = pl.ds(pl.multiple_of(r * 16, 16), 16)
                for k in range(TILES):
                    place = (at, pl.ds(k * across, across))
                    move(place, g_ref[place])

        for one in stores(n):
            one.start()
    for n in range(max(0, len(items) - SLOTS), len(items)):
        for one in stores(n):
            one.wait()


def place():
    me = lax.axis_index("dp")
    return me % 2, me // 2


def spot(c, x, core, rel):
    near = x + (rel % 2) * (1 - 2 * (x % 2))
    return (c + core) % 2 * 4 + (3 - near if rel // 2 else near)


def update(factor, items, gs, old, new):
    rows, cols = old[0].shape[1:]
    tiles, down_rows, down_cols = old[2].shape[1:]
    wide, tall = (rows // 16, cols), (tiles, down_rows // 8, down_cols // 2)
    bf16, wider = jnp.bfloat16, jnp.float32

    def slots(shape):
        return [pltpu.VMEM((SLOTS, *one), t) for one, t in ((shape, bf16), (shape, wider), (shape, wider), (wide, bf16))]

    any_spec = pl.BlockSpec(memory_space=pl.ANY)
    n_in = 1 + len(gs) + 9 + (9 if new is not None else 0)
    size = len(items) * wide[0] * wide[1]
    return pl.pallas_call(
        functools.partial(update_kernel, items, new is None),
        out_shape=[jax.ShapeDtypeStruct(o.shape, o.dtype) for o in old],
        in_specs=[any_spec] * n_in,
        out_specs=[any_spec] * 9,
        scratch_shapes=[
            pltpu.VMEM((8, 128), jnp.float32),
            slots(wide),
            slots(tall),
            pltpu.SemaphoreType.DMA((4, SLOTS)),
            pltpu.SemaphoreType.DMA((3, SLOTS)),
            pltpu.SemaphoreType.DMA,
        ],
        input_output_aliases={} if new is None else {n_in - 9 + i: i for i in range(9)},
        cost_estimate=pl.CostEstimate(flops=size * 400, bytes_accessed=size * 22, transcendentals=size),
        compiler_params=pltpu.CompilerParams(vmem_limit_bytes=62 * 2**20),
    )(factor, *gs, *old, *(new if new is not None else ()))


def solution(mesh):
    n = mesh.shape["dp"]
    chips = n // 2
    pair_a = [(2 * x + c, 2 * (x ^ 1) + c) for x in range(chips) for c in range(2)]
    pair_b = [(2 * x + c, 2 * (chips - 1 - x) + c) for x in range(chips) for c in range(2)]
    peers = [(i, i ^ 1) for i in range(n)]
    to_a, to_b, to_peer = (functools.partial(lax.ppermute, axis_name="dp", perm=perm) for perm in (pair_a, pair_b, peers))

    def gather(shards, factor, arrays):
        layers = arrays[0].shape[0]
        calls = []

        arrays = [w.reshape(layers, TILES, w.shape[1] // TILES, w.shape[2]) if i % 3 == 2 else w for i, w in enumerate(arrays)]

        def run(new, parts):
            items = []
            for i, (unit, _, core, rel) in enumerate(parts):
                number, colour, _ = shards[unit]
                items += [(i, mat, mat, number, core, rel, colour) for mat in range(3)]
            calls.append(len(calls))
            return update(factor, items, [g for _, g, _, _ in parts], arrays, new)

        def after(new, waited):
            first, waited = lax.optimization_barrier((new[0], waited))
            return [first, *new[1:]], waited

        near = []
        for _, _, own in shards:
            one = to_a(own)
            near.append((one, to_b(own)))
        beside = [to_peer(own) for _, _, own in shards]
        new = run(None, [(u, own, 0, 0) for u, (_, _, own) in enumerate(shards)] + [(u, g, 1, 0) for u, g in enumerate(beside)])
        far, waiting = [], []
        for u, (_, colour, _) in enumerate(shards):
            new, got = after(new, near[u])
            far.append(to_b(got[0]) if colour else to_a(got[1]))
            across = [(u, to_peer(g), 1, 1 + j) for j, g in enumerate(got)]
            new = run(new, [(u, g, 0, 1 + j) for j, g in enumerate(got)] + waiting)
            waiting = across
        for u, g in enumerate(far):
            new, got = after(new, g)
            across = [(u, to_peer(got), 1, 3)]
            new = run(new, waiting + [(u, got, 0, 3)])
            waiting = across
        new = run(new, waiting)
        return new

    def step(x, dy, *arrays):
        weights = arrays[:3]
        layers = weights[0].shape[0]
        blocks, factor = backward(n, x[0], dy[0], weights)
        shards = [(number, colour, blocks[2 * number + colour]) for number in reversed(range(layers)) for colour in range(2)]

        new = gather(shards, factor, arrays)
        new = [o.reshape(o.shape[0], -1, o.shape[-1]) for o in new]
        return tuple(new)

    return jax.shard_map(
        step,
        mesh=mesh,
        in_specs=(P(("rep", "dp"), None, None),) * 2 + (P(None, None, None),) * 9,
        out_specs=(P("rep", None, None),) * 9,
        check_vma=False,
    )
```

```python
import functools

import jax
import jax.numpy as jnp
from jax import lax
from jax.experimental import pallas as pl
from jax.experimental.pallas import tpu as pltpu
from jax.sharding import PartitionSpec as P


SLOTS = 6


MESH = pl.DeviceIdType.MESH
DEEP = 4
TILES = 5


def hops():
    me = lax.axis_index("dp")
    c, x = me % 2, me // 2
    a = x + 1 - 2 * (x % 2)
    return me, c, x, a, 3 - x, 3 - a


def backward_kernel(
    n, layers, x_ref, dy_ref, wg_ref, wu_ref, wd_ref, *refs
):
    outs, besides, factor_ref, refs = refs[: 2 * layers], refs[2 * layers : 4 * layers], refs[4 * layers], refs[4 * layers + 1 :]
    (hs, a, aT, dh, wg, wu, wd, actT, dgate, dup, acc_g, acc_u, send0, own, rcv0, rcv1, rcv2, fin, squares, parts,
     w_sem, h_sem, send0_sem, rcv0_sem, send1_sem, rcv1_sem, send2_sem, rcv2_sem, fin_sem, bsend_sem, brecv_sem, ssend_sem, srecv_sem,
     credit_p, credit_a, credit_b) = refs
    me, c, x, xa, xb, xo = hops()
    peer, to_a, to_b = 2 * x + 1 - c, 2 * xa + c, 2 * xb + c
    tokens, depth = dh.shape
    width, broad, hidden = dgate.shape[-1], wg.shape[-1], wg_ref.shape[-1]
    many, rest = hidden // broad, hidden % broad
    steps = layers * TILES
    half = depth // 2
    ahead = (layers - 1) * (many + 1)
    tall = 512

    def piece(t, number, start, size):
        slot, at, here = t % 2, pl.ds(start, size), pl.ds(0, size)
        return [
            pltpu.make_async_copy(wg_ref.at[number, :, at], wg.at[slot, :, here], w_sem.at[0, slot]),
            pltpu.make_async_copy(wu_ref.at[number, :, at], wu.at[slot, :, here], w_sem.at[1, slot]),
            pltpu.make_async_copy(wd_ref.at[number, at], wd.at[slot, here], w_sem.at[2, slot]),
        ]

    def weights_of(s):
        return piece(s + ahead, layers - 1 - s // TILES, pl.multiple_of(s % TILES * width, 128), width)

    def turn(source, target):
        @pl.loop(0, tokens // 128)
        def _(r):
            at = pl.ds(pl.multiple_of(r * 128, 128), 128)
            target[:, at] = source[at, :].T

    def norm(h):
        @pl.loop(0, tokens // 64)
        def _(r):
            at = pl.ds(pl.multiple_of(r * 64, 64), 64)
            wide = h[at].astype(jnp.float32)
            scale = lax.rsqrt(jnp.mean(wide**2, -1, keepdims=True) + 1e-6)
            a[at] = (wide * scale).astype(jnp.bfloat16)

    first_h = pltpu.make_async_copy(x_ref, hs.at[0], h_sem.at[0])
    first_h.start()
    first_dh = pltpu.make_async_copy(dy_ref, dh, h_sem.at[1])
    first_dh.start()
    for one in piece(0, 0, 0, broad):
        one.start()

    barrier = pltpu.get_barrier_semaphore()
    for k in range(1, n):
        pl.semaphore_signal(barrier, inc=1, device_id={"dp": (me + k) % n}, device_id_type=MESH)
    pl.semaphore_wait(barrier, n - 1)

    first_h.wait()

    for number in range(layers - 1):
        norm(hs.at[number])
        acc_g[...] = jnp.zeros_like(acc_g)

        base = number * (many + 1)

        def onward(slot, size):
            here = pl.ds(0, size)

            @pl.loop(0, tokens // tall)
            def _(r):
                at = pl.ds(pl.multiple_of(r * tall, tall), tall)
                gate = jnp.dot(a[at], wg[slot, :, here], preferred_element_type=jnp.float32)
                up = jnp.dot(a[at], wu[slot, :, here], preferred_element_type=jnp.float32)
                hot = (gate * jax.nn.sigmoid(gate) * up).astype(jnp.bfloat16)
                acc_g[at] += jnp.dot(hot, wd[slot, here], preferred_element_type=jnp.float32)

        @pl.loop(0, many)
        def _(i):
            for one in piece(base + i, number, pl.multiple_of(i * broad, 128), broad):
                one.wait()

            @pl.when(i + 1 < many)
            def _():
                for one in piece(base + i + 1, number, pl.multiple_of((i + 1) * broad, 128), broad):
                    one.start()

            @pl.when(i + 1 == many)
            def _():
                for one in piece(base + many, number, many * broad, rest):
                    one.start()

            onward((base + i) % 2, broad)

        for one in piece(base + many, number, many * broad, rest):
            one.wait()
        for one in weights_of(0) if number == layers - 2 else piece(base + many + 1, number + 1, 0, broad):
            one.start()
        onward((base + many) % 2, rest)

        @pl.loop(0, tokens // 64)
        def _(r):
            at = pl.ds(pl.multiple_of(r * 64, 64), 64)
            hs[number + 1, at] = hs[number, at] + acc_g[at].astype(jnp.bfloat16)

    norm(hs.at[layers - 1])
    turn(a, aT)
    first_dh.wait()

    def remote(source, target, sends, receives, to):
        return pltpu.make_async_remote_copy(
            src_ref=source, dst_ref=target, send_sem=sends, recv_sem=receives, device_id={"dp": to}, device_id_type=MESH
        )

    def swap(s):
        return remote(send0.at[s % 2], rcv0.at[s % DEEP], send0_sem.at[s % 2], rcv0_sem.at[s % DEEP], peer)

    def step_one(s):
        k = s % DEEP
        blocks = ((2 * xa, to_a), (2 * xo, to_a), (2 * xb + 1, to_b), (2 * xo + 1, to_b))
        return [(b, remote(own.at[k, b], rcv1.at[k, i], send1_sem.at[k, i], rcv1_sem.at[k, i], to)) for i, (b, to) in enumerate(blocks)]

    def step_two(s):
        k = s % DEEP
        blocks = ((2 * xb, to_b, 1), (2 * xa + 1, to_a, 3))
        return [
            (b, got, remote(own.at[k, b], rcv2.at[k, i], send2_sem.at[k, i], rcv2_sem.at[k, i], to)) for i, (b, to, got) in enumerate(blocks)
        ]

    def summed(s, b, more):
        k = s % DEEP
        for mat in range(3):
            for r in range(0, own.shape[-2], 16):
                at = pl.ds(r, 16)
                total = own[k, b, mat, at].astype(jnp.float32) + rcv0[k, b, mat, at].astype(jnp.float32)
                for ref, i in more:
                    total = total + ref[k, i, mat, at].astype(jnp.float32)
                yield mat, at, total.astype(jnp.bfloat16)

    def begin(s):
        swap(s).wait_recv()

        @pl.when(s >= DEEP)
        def _():
            pl.semaphore_wait(credit_a, 1)
            pl.semaphore_wait(credit_b, 1)

        copies = step_one(s)
        for b, _ in copies:
            for mat, at, total in summed(s, b, ()):
                own[s % DEEP, b, mat, at] = total
        for _, one in copies:
            one.start()

    def pass_on(s):
        for _, one in step_one(s):
            one.wait_recv()
        copies = step_two(s)
        for b, got, _ in copies:
            for mat, at, total in summed(s, b, ((rcv1, got),)):
                own[s % DEEP, b, mat, at] = total
        for *_, one in copies:
            one.start()

    def fin_copies(s, number):
        at = pl.ds(pl.multiple_of((s % TILES) * width, width), width)
        return [pltpu.make_async_copy(fin.at[colour], outs[2 * number + colour].at[:, :, at], fin_sem.at[colour]) for colour in range(2)]

    def over(s, number):
        at = pl.ds(pl.multiple_of((s % TILES) * width, width), width)
        return [
            remote(fin.at[colour], besides[2 * number + colour].at[:, :, at], bsend_sem.at[colour], brecv_sem.at[s, colour], peer)
            for colour in range(2)
        ]

    def finish(s):
        for *_, one in step_two(s):
            one.wait_recv()

        @pl.when(s >= 1)
        def _():
            for one in fin_copies(s, 0):
                one.wait()
            for one in over(s, 0):
                one.wait_send()

        for colour in range(2):
            for mat, at, total in summed(s, 2 * x + colour, ((rcv1, 2 * colour), (rcv2, colour))):
                fin[colour, mat, at] = total
                squared = total.astype(jnp.float32) ** 2
                squares[...] += squared[:8] + squared[8:]
        for number in range(layers):

            @pl.when(layers - 1 - s // TILES == number)
            def _():
                for one in fin_copies(s, number) + over(s, number):
                    one.start()

        for _, one in step_one(s):
            one.wait_send()
        for *_, one in step_two(s):
            one.wait_send()

        @pl.when(s + DEEP < steps)
        def _():
            pl.semaphore_signal(credit_p, inc=1, device_id={"dp": peer}, device_id_type=MESH)
            pl.semaphore_signal(credit_a, inc=1, device_id={"dp": to_a}, device_id_type=MESH)
            pl.semaphore_signal(credit_b, inc=1, device_id={"dp": to_b}, device_id_type=MESH)

    def gradients(core, keep):
        for_rows = half // tall

        @pl.loop(0, for_rows)
        def _(r):
            at = pl.ds(pl.multiple_of(core * half + r * tall, tall), tall)
            blocks = tall // 64
            for mat, right in enumerate((dgate, dup)):
                got = jnp.dot(aT[at], right[...], preferred_element_type=jnp.float32).astype(jnp.bfloat16)
                for b in range(blocks):
                    keep((r * blocks + b, mat), got[b * 64 : (b + 1) * 64])
            rows = width // 2 // for_rows
            at = pl.ds(pl.multiple_of(core * (width // 2) + r * rows, rows), rows)
            got = jnp.dot(actT[at], dh[...], preferred_element_type=jnp.float32).astype(jnp.bfloat16)
            rows = width // 8
            for b in range(blocks):
                for i in range(rows // 16):
                    for k in range(4):
                        row, col = b // 2 * rows + i * 16, b % 2 * (depth // 2) + k * 128
                        place = (r * blocks + b, 2, pl.ds(k * 16, 16), pl.ds(i * 128, 128))
                        keep(place, got[row : row + 16, col : col + 128])

    squares[...] = jnp.zeros_like(squares)

    @pl.loop(0, steps)
    def _(s):
        slot, even, k = (s + ahead) % 2, s % 2, s % DEEP
        here = pl.ds(0, width)
        for one in weights_of(s):
            one.wait()

        @pl.when(s + 1 < steps)
        def _():
            for one in weights_of(s + 1):
                one.start()

        @pl.loop(0, tokens // tall)
        def _(r):
            at = pl.ds(pl.multiple_of(r * tall, tall), tall)
            gate = jnp.dot(a[at], wg[slot, :, here], preferred_element_type=jnp.float32)
            up = jnp.dot(a[at], wu[slot, :, here], preferred_element_type=jnp.float32)
            by_act = lax.dot_general(dh[at], wd[slot, here], (((1,), (1,)), ((), ())), preferred_element_type=jnp.float32)
            by_act = by_act.astype(jnp.bfloat16).astype(jnp.float32)
            share = jax.nn.sigmoid(gate)
            silu = gate * share
            actT[:, at] = (silu * up).astype(jnp.bfloat16).T
            dup[at] = (by_act * silu).astype(jnp.bfloat16)
            dgate[at] = (by_act * up * (share + silu * (1.0 - share))).astype(jnp.bfloat16)

        @pl.when(s >= 2)
        def _():
            swap(s).wait_send()

        def to_send(place, value):
            send0[even, *place] = value

        gradients(1 - c, to_send)

        @pl.when(s >= DEEP)
        def _():
            pl.semaphore_wait(credit_p, 1)

        swap(s).start()

        def to_own(place, value):
            own[k, *place] = value

        gradients(c, to_own)
        begin(s)

        @pl.when(s >= 1)
        def _():
            pass_on(s - 1)

        @pl.when(s >= DEEP - 1)
        def _():
            finish(s - (DEEP - 1))

        @pl.when(s < steps - TILES)
        def _():
            @pl.when(s % TILES == 0)
            def _():
                acc_g[...] = jnp.zeros_like(acc_g)
                acc_u[...] = jnp.zeros_like(acc_u)

            @pl.loop(0, tokens // tall)
            def _(r):
                at = pl.ds(pl.multiple_of(r * tall, tall), tall)
                for total, by, w in ((acc_g, dgate, wg), (acc_u, dup, wu)):
                    total[at] += lax.dot_general(by[at], w[slot, :, here], (((1,), (1,)), ((), ())), preferred_element_type=jnp.float32)

            @pl.when(s % TILES == TILES - 1)
            def _():
                @pl.loop(0, tokens // 32)
                def _(r):
                    at = pl.ds(pl.multiple_of(r * 32, 32), 32)
                    by = acc_g[at].astype(jnp.bfloat16) + acc_u[at].astype(jnp.bfloat16)
                    by, wide = by.astype(jnp.float32), hs[layers - 1 - s // TILES, at].astype(jnp.float32)
                    scale = lax.rsqrt(jnp.mean(wide**2, -1, keepdims=True) + 1e-6)
                    inner = jnp.mean(by * wide, -1, keepdims=True)
                    by_h = (by * scale - wide * (scale * scale * scale * inner)).astype(jnp.bfloat16)
                    dh[at] = dh[at] + by_h

                norm(hs.at[layers - 2 - s // TILES])
                turn(a, aT)

    pass_on(jnp.int32(steps - 1))
    for back in range(DEEP - 1, 0, -1):
        finish(jnp.int32(steps - back))
    for one in fin_copies(jnp.int32(steps - 1), 0):
        one.wait()
    for one in over(jnp.int32(steps - 1), 0):
        one.wait_send()
    swap(jnp.int32(steps - 2)).wait_send()
    swap(jnp.int32(steps - 1)).wait_send()

    parts[me] = sum(squares[:, k * 128 : (k + 1) * 128] for k in range(width // 128))

    def share(k):
        return remote(parts.at[me], parts.at[me], ssend_sem.at[k], srecv_sem.at[k], (me + k) % n)

    for k in range(1, n):
        share(k).start()
    for s in range(steps):
        for one in over(s, layers - 1 - s // TILES):
            one.wait_recv()
    for k in range(1, n):
        share(k).wait()
    total = parts[0]
    for k in range(1, n):
        total = total + parts[k]
    count = steps * width * depth * 3
    factor_ref[...] = jnp.minimum(1.0, 0.5 * lax.rsqrt(jnp.full(factor_ref.shape, jnp.sum(total)) / count + 1e-30))


def backward(n, x, dy, weights):
    layers, depth, hidden = weights[0].shape
    tokens, width, rows = dy.shape[0], hidden // TILES, depth // 16
    broad = (width // 256 + 1) * 256
    bf16, dma, regular = jnp.bfloat16, pltpu.SemaphoreType.DMA, pltpu.SemaphoreType.REGULAR
    any_spec = pl.BlockSpec(memory_space=pl.ANY)
    out = pl.pallas_call(
        functools.partial(backward_kernel, n, layers),
        out_shape=[jax.ShapeDtypeStruct((3, rows, hidden), bf16)] * (4 * layers)
        + [jax.ShapeDtypeStruct((8, 128), jnp.float32)],
        in_specs=[any_spec] * 5,
        out_specs=[any_spec] * (4 * layers) + [pl.BlockSpec(memory_space=pltpu.VMEM)],
        scratch_shapes=[
            pltpu.VMEM((layers, tokens, depth), bf16),
            pltpu.VMEM((tokens, depth), bf16),
            pltpu.VMEM((depth, tokens), bf16),
            pltpu.VMEM((tokens, depth), bf16),
            pltpu.VMEM((2, depth, broad), bf16),
            pltpu.VMEM((2, depth, broad), bf16),
            pltpu.VMEM((2, broad, depth), bf16),
            pltpu.VMEM((width, tokens), bf16),
            pltpu.VMEM((tokens, width), bf16),
            pltpu.VMEM((tokens, width), bf16),
            pltpu.VMEM((tokens, depth), jnp.float32),
            pltpu.VMEM((tokens, depth), jnp.float32),
            pltpu.VMEM((2, 8, 3, rows, width), bf16),
            pltpu.VMEM((DEEP, 8, 3, rows, width), bf16),
            pltpu.VMEM((DEEP, 8, 3, rows, width), bf16),
            pltpu.VMEM((DEEP, 4, 3, rows, width), bf16),
            pltpu.VMEM((DEEP, 2, 3, rows, width), bf16),
            pltpu.VMEM((2, 3, rows, width), bf16),
            pltpu.VMEM((8, width), jnp.float32),
            pltpu.VMEM((n, 8, 128), jnp.float32),
            dma((3, 2)),
            dma((2,)),
            dma((2,)),
            dma((DEEP,)),
            dma((DEEP, 4)),
            dma((DEEP, 4)),
            dma((DEEP, 2)),
            dma((DEEP, 2)),
            dma((2,)),
            dma((2,)),
            dma((layers * TILES, 2)),
            dma((n,)),
            dma((n,)),
            regular,
            regular,
            regular,
        ],
        compiler_params=pltpu.CompilerParams(collective_id=0, has_side_effects=True, vmem_limit_bytes=67_043_328),
        cost_estimate=pl.CostEstimate(flops=16 * tokens * depth * hidden * layers, bytes_accessed=2**27, transcendentals=0),
    )(x, dy, *weights)
    return out[: 2 * layers], out[2 * layers : -1], out[-1]


def update_kernel(items, n_new, *refs):
    n_g = 1 + max(item[0] for item in items)
    factor_ref, refs = refs[0], refs[1:]
    g_refs, refs = refs[:n_g], refs[n_g:]
    old, refs = refs[:9], refs[9:]
    if not n_new:
        refs = refs[9:]
    new, refs = refs[:9], refs[9:]
    factor_vmem, wide, tall, in_sem, out_sem, f_sem = refs
    c, x = place()
    copy = pltpu.make_async_copy(factor_ref, factor_vmem, f_sem)
    copy.start()

    def views(n):
        which, tile, weight, layer, core, rel, colour = items[n]
        slot = n % SLOTS
        buffers = [b.at[slot] for b in (tall if weight == 2 else wide)]
        owner = spot(c, x, core, rel)
        if weight == 2:
            rows, cols = buffers[0].shape[1:]
            index = (layer, slice(None), pl.ds(pl.multiple_of(owner * rows, rows), rows), pl.ds(colour * cols, cols))
        else:
            rows = buffers[0].shape[0]
            index = (layer, pl.ds(pl.multiple_of((owner * 2 + colour) * rows, rows), rows))
        sources = [old[3 * j + weight].at[index] for j in range(3)] + [g_refs[which].at[tile]]
        targets = [new[3 * j + weight].at[index] for j in range(3)]
        return buffers, sources, targets, slot

    def loads(n):
        buffers, sources, _, slot = views(n)
        return [pltpu.make_async_copy(s, b, in_sem.at[j, slot]) for j, (s, b) in enumerate(zip(sources, buffers, strict=True))]

    def stores(n):
        buffers, _, targets, slot = views(n)
        return [pltpu.make_async_copy(b, t, out_sem.at[j, slot]) for j, (b, t) in enumerate(zip(buffers[:3], targets, strict=True))]

    ahead = SLOTS - 2
    for n in range(min(ahead, len(items))):
        for one in loads(n):
            one.start()
    copy.wait()
    factor = factor_vmem[0:1, 0:1]
    for n in range(len(items)):
        if n + ahead < len(items):
            if n + ahead - SLOTS >= 0:
                for one in stores(n + ahead - SLOTS):
                    one.wait()
            for one in loads(n + ahead):
                one.start()
        for one in loads(n):
            one.wait()
        w_ref, m_ref, v_ref, g_ref = views(n)[0]

        def move(place, g):
            g = g.astype(jnp.float32) * factor
            m = 0.9 * m_ref[place] + 0.1 * g
            v = 0.95 * v_ref[place] + 0.05 * g * g
            w = w_ref[place].astype(jnp.float32)
            step = m * lax.rsqrt(v + 1e-8) + 0.1 * w
            w_ref[place] = (w - 0.02 * step).astype(jnp.bfloat16)
            m_ref[place] = m
            v_ref[place] = v

        if items[n][2] == 2:
            tiles, rows = w_ref.shape[:2]

            @pl.loop(0, tiles * (rows // 16))
            def _(r):
                for k in range(g_ref.shape[0] // 16):
                    place = (r // (rows // 16), pl.ds(pl.multiple_of(r % (rows // 16) * 16, 16), 16), pl.ds(k * 128, 128))
                    move(place, g_ref[pl.ds(k * 16, 16), pl.ds(pl.multiple_of(r * 128, 128), 128)])
        else:
            rows, cols = w_ref.shape
            across = cols // TILES

            @pl.loop(0, rows // 16)
            def _(r):
                at = pl.ds(pl.multiple_of(r * 16, 16), 16)
                for k in range(TILES):
                    place = (at, pl.ds(k * across, across))
                    move(place, g_ref[place])

        for one in stores(n):
            one.start()
    for n in range(max(0, len(items) - SLOTS), len(items)):
        for one in stores(n):
            one.wait()


def place():
    me = lax.axis_index("dp")
    return me % 2, me // 2


def spot(c, x, core, rel):
    near = x + (rel % 2) * (1 - 2 * (x % 2))
    return (c + core) % 2 * 4 + (3 - near if rel // 2 else near)


def update(factor, items, gs, old, new):
    rows, cols = old[0].shape[1:]
    tiles, down_rows, down_cols = old[2].shape[1:]
    wide, tall = (rows // 16, cols), (tiles, down_rows // 8, down_cols // 2)
    bf16, wider = jnp.bfloat16, jnp.float32

    def slots(shape):
        return [pltpu.VMEM((SLOTS, *one), t) for one, t in ((shape, bf16), (shape, wider), (shape, wider), (wide, bf16))]

    any_spec = pl.BlockSpec(memory_space=pl.ANY)
    n_in = 1 + len(gs) + 9 + (9 if new is not None else 0)
    size = len(items) * wide[0] * wide[1]
    return pl.pallas_call(
        functools.partial(update_kernel, items, new is None),
        out_shape=[jax.ShapeDtypeStruct(o.shape, o.dtype) for o in old],
        in_specs=[any_spec] * n_in,
        out_specs=[any_spec] * 9,
        scratch_shapes=[
            pltpu.VMEM((8, 128), jnp.float32),
            slots(wide),
            slots(tall),
            pltpu.SemaphoreType.DMA((4, SLOTS)),
            pltpu.SemaphoreType.DMA((3, SLOTS)),
            pltpu.SemaphoreType.DMA,
        ],
        input_output_aliases={} if new is None else {n_in - 9 + i: i for i in range(9)},
        cost_estimate=pl.CostEstimate(flops=size * 400, bytes_accessed=size * 22, transcendentals=size),
        compiler_params=pltpu.CompilerParams(vmem_limit_bytes=62 * 2**20),
    )(factor, *gs, *old, *(new if new is not None else ()))


def solution(mesh):
    n = mesh.shape["dp"]
    chips = n // 2
    pair_a = [(2 * x + c, 2 * (x ^ 1) + c) for x in range(chips) for c in range(2)]
    pair_b = [(2 * x + c, 2 * (chips - 1 - x) + c) for x in range(chips) for c in range(2)]
    peers = [(i, i ^ 1) for i in range(n)]
    to_a, to_b, to_peer = (functools.partial(lax.ppermute, axis_name="dp", perm=perm) for perm in (pair_a, pair_b, peers))

    def gather(shards, beside, factor, arrays):
        layers = arrays[0].shape[0]
        calls = []

        arrays = [w.reshape(layers, TILES, w.shape[1] // TILES, w.shape[2]) if i % 3 == 2 else w for i, w in enumerate(arrays)]

        def run(new, parts):
            items = []
            for i, (unit, _, core, rel) in enumerate(parts):
                number, colour, _ = shards[unit]
                items += [(i, mat, mat, number, core, rel, colour) for mat in range(3)]
            calls.append(len(calls))
            return update(factor, items, [g for _, g, _, _ in parts], arrays, new)

        def after(new, waited):
            first, waited = lax.optimization_barrier((new[0], waited))
            return [first, *new[1:]], waited

        near = []
        for _, _, own in shards:
            one = to_a(own)
            near.append((one, to_b(own)))
        new = run(None, [(u, own, 0, 0) for u, (_, _, own) in enumerate(shards)] + [(u, g, 1, 0) for u, g in enumerate(beside)])
        far, waiting = [], []
        for u, (_, colour, _) in enumerate(shards):
            if u >= 2:
                new, waiting = run(new, waiting), []
            new, got = after(new, near[u])
            far.append(to_b(got[0]) if colour else to_a(got[1]))
            across = [(u, to_peer(g), 1, 1 + j) for j, g in enumerate(got)]
            new = run(new, [(u, g, 0, 1 + j) for j, g in enumerate(got)] + waiting)
            waiting = across
        for u in range(0, len(far), 2):
            new = run(new, waiting)
            new, got = after(new, far[u : u + 2])
            got = list(enumerate(got, u))
            across = [(i, to_peer(g), 1, 3) for i, g in got]
            new = run(new, [(i, g, 0, 3) for i, g in got])
            waiting = across
        new = run(new, waiting)
        return new

    def step(x, dy, *arrays):
        weights = arrays[:3]
        layers = weights[0].shape[0]
        blocks, besides, factor = backward(n, x[0], dy[0], weights)
        shards, beside = [], []
        for number in reversed(range(layers)):
            for colour in range(2):
                shards.append((number, colour, blocks[2 * number + colour]))
                beside.append(besides[2 * number + colour])

        new = gather(shards, beside, factor, arrays)
        new = [o.reshape(o.shape[0], -1, o.shape[-1]) for o in new]
        return tuple(new)

    return jax.shard_map(
        step,
        mesh=mesh,
        in_specs=(P(("rep", "dp"), None, None),) * 2 + (P(None, None, None),) * 9,
        out_specs=(P("rep", None, None),) * 9,
        check_vma=False,
    )
```
